32 devices in a mesh: ga: 8 (over z, y), ba: 4 (over x, core).
Axes of the slice: x: 2, y: 2, z: 4, core: 2. Of those that a mesh axis runs over, the one named last changes fastest.
Arguments:
- coefficients: bfloat16 [10240, 6144], P('ga', 'ba')
- rotation: bfloat16 [6144, 6144], P('ga', 'ba'), may hold values from -0.078125 to 0.078125
Outputs:
- new_coefficients: bfloat16 [10240, 6144], P('ga', 'ba')
- band_rms: float32 [6144], P('ba')
The draws below stay inside these ranges and needn't reach their ends.
All inputs are finite; a program needn't handle non-finite values.
Results may differ from the reference program's by a relative error of at most 0.0004.
Values may be sent and summed in bfloat16 or wider, within the bound.
A program may use at most 128 MiB of HBM per device.

```python
import math
import jax
import jax.numpy as jnp
from jax import lax

NB = 6144
NG = 10240


def draw_coefficients(key, part):
    first, second, third = jax.random.split(jax.random.fold_in(key, 11), 3)
    positions = jnp.arange(NG, dtype=jnp.float32)[:, None]
    row_scale = jnp.exp(positions / NG * math.log(3.0)) * jnp.exp(jax.random.uniform(first, (NG, 1), jnp.float32) * math.log(3.3))
    col_scale = jnp.exp(jax.random.uniform(second, (1, NB), jnp.float32) * math.log(10.0))
    base = jnp.clip(jax.random.normal(third, (NG, NB), jnp.float32), -6.0, 6.0)
    return (base * row_scale * col_scale).astype(jnp.bfloat16)


def steps_of(own_key, shape, shards, least, largest):
    loudness = 1.0
    for axis_at, parts in shards:
        heights = jax.random.uniform(jax.random.fold_in(jax.random.fold_in(own_key, 6), axis_at), (parts,), jnp.float32, least / len(shards), largest / len(shards))
        loudness = loudness * jnp.repeat(jnp.exp(heights), shape[axis_at] // parts).reshape((-1,) + (1,) * (len(shape) - 1 - axis_at))
    return loudness


def normal_values(own_key, shape, deviation, limit, shards=(), kind=jnp.bfloat16):
    drawn = jax.random.normal(own_key, shape, jnp.float32) * deviation
    if len(shards) > 0:
        drawn = steps_of(own_key, shape, shards, -0.22, 0.18) * drawn
    return jnp.clip(drawn, min=-limit, max=limit).astype(kind)


def setup_inputs(seed: int = 0) -> dict:
    seeds = jax.random.split(jax.random.key(seed), 3)
    coefficients = draw_coefficients(jax.random.fold_in(seeds[2], 71), 0)
    rotation = normal_values(seeds[1], (NB, NB), NB ** -0.5, 0.078125, ((0, 8), (1, 4)))
    return {"coefficients": coefficients, "rotation": rotation}


def reference(coefficients, rotation):
    rotated = jnp.dot(coefficients, rotation, preferred_element_type=jnp.float32)
    sums = lax.optimization_barrier(jnp.sum(rotated * rotated, axis=0))
    band_rms = jnp.sqrt(sums / NG + 1e-06)
    return ((rotated / band_rms).astype(jnp.bfloat16), band_rms)
```

```python
import functools
import math

import jax
import jax.numpy as jnp
from jax import lax
from jax.experimental import pallas as pl
from jax.experimental.pallas import tpu as pltpu
from jax.sharding import PartitionSpec as P

MESH = pl.DeviceIdType.MESH
CHUNKS = 6
CROSS = 1
LENT = 6


def kernel(n_ga, n_ba, line, coef, rot, total, rms_out, a_buf, b_buf, stats,
           recv, send_z, send_zb, send_y, a_recv, a_send_x, a_send_p, s_recv, s_send, own):
    lanes = n_ga // line
    depth = rot.shape[0]
    rows, width = coef.shape
    piece = depth // CHUNKS
    span = lanes * depth
    me, mb = lax.axis_index("ga"), lax.axis_index("ba")
    z, w = me // lanes, lax.rem(me, lanes)
    bx, bc = mb // 2, lax.rem(mb, 2)
    half = n_ba // 2

    def ga(i):
        return {"ga": i}

    def side(o):
        return lax.rem(w + o, lanes)

    def chunk(index):
        return b_buf.at[pl.ds(pl.multiple_of(index * piece, piece), piece)]

    partner = mb + 1 - 2 * bc
    far = [lax.rem(bx + o, half) * 2 + bc for o in range(1, half)]

    barrier = pltpu.get_barrier_semaphore()
    def greet(device):
        pl.semaphore_signal(barrier, inc=1, device_id=device, device_id_type=MESH)

    @pl.when(z > 0)
    def _():
        greet(ga(me - lanes))

    @pl.when(z < line - 1)
    def _():
        greet(ga(me + lanes))

    for o in range(1, lanes):
        greet(ga(z * lanes + side(o)))
    for target in [*far, partner]:
        greet({"ba": target})

    mine = [
        pltpu.make_async_copy(rot, b_buf.at[pl.ds(pl.multiple_of(me * depth, depth), depth)], own.at[0]),
        pltpu.make_async_copy(coef, a_buf.at[mb], own.at[1]),
    ]
    ends = (line - 1 - z) // (line - 1) + z // (line - 1)
    pl.semaphore_wait(barrier, 2 - ends + lanes - 1 + len(far) + 1)

    def remote(src, index, sem, target):
        return pltpu.make_async_remote_copy(
            src_ref=src, dst_ref=chunk(index), send_sem=sem, recv_sem=recv.at[index],
            device_id=ga(target), device_id_type=MESH)

    def arrived(index):
        pltpu.make_async_copy(chunk(index), chunk(index), recv.at[index]).wait()

    def along(k, src, index, sem):
        @pl.when(z < line - 1 if k == 0 else z > 0)
        def _():
            remote(src, index, sem, me + lanes if k == 0 else me - lanes).start()

    def across(src, index, from_z):
        for o in range(1, lanes):
            remote(src, index, send_y.at[o - 1, from_z], z * lanes + side(o)).start()

    def own_chunk(q):
        return rot.at[pl.ds(q * piece, piece)]

    last = CHUNKS - CROSS
    crossed = [(o, q) for q in range(last, CHUNKS) for o in range(1, lanes)]
    for q in range(last, CHUNKS):
        across(own_chunk(q), me * CHUNKS + q, z)
    for q in range(CHUNKS):
        for k in range(2):
            along(k, own_chunk(q), me * CHUNKS + q, send_z.at[k, z])
        if q < last:
            across(own_chunk(q), me * CHUNKS + q, z)

    def a_copy(src, index, sem, target):
        return pltpu.make_async_remote_copy(
            src_ref=src, dst_ref=a_buf.at[index], send_sem=sem, recv_sem=a_recv.at[index],
            device_id={"ba": target}, device_id_type=MESH)

    for o, target in enumerate(far):
        a_copy(coef, mb, a_send_x.at[o], target).start()
    a_copy(coef, mb, a_send_p.at[mb], partner).start()
    for copy in mine:
        copy.start()

    for o, q in crossed:
        index = (z * lanes + side(o)) * CHUNKS + q
        arrived(index)
        for k in range(2):
            along(k, chunk(index), index, send_zb.at[k, z * lanes + side(o)])

    tile = math.gcd(rows, 1280)

    def multiply(j, dist, part):
        from_z = z - dist + 2 * dist * j

        @pl.when((from_z >= 0) & (from_z < line) & ((dist > 0) | (j == 0)))
        def _():
            if part == "all":
                for o in range(1, lanes):
                    for q in range(last):
                        arrived((from_z * lanes + side(o)) * CHUNKS + q)
                panel(from_z * span, span, dist)
                return
            if part == "own":
                panel((from_z * lanes + w) * depth, depth, dist)
                return
            for o in range(1, lanes):
                block = from_z * lanes + side(o)
                for q in range(cut) if part == "cut" else range(cut, last):
                    arrived(block * CHUNKS + q)
                if part == "cut":
                    panel(block * depth, cut * piece, dist)
                else:
                    panel(block * depth + cut * piece, depth - cut * piece, dist)

    cut = max(q for q in range(last) if q * piece % 128 == 0) if depth % 128 == 0 else 0

    def panel(begin, size, dist):
        at, column = begin // width, pl.multiple_of(lax.rem(begin, width), 128)

        @pl.loop(0, rows // tile)
        def _(t):
            part = pl.ds(pl.multiple_of(t * tile, tile), tile)
            product = jnp.dot(
                a_buf[at, part, pl.ds(column, size)],
                b_buf[pl.ds(pl.multiple_of(begin, 128), size), :],
                preferred_element_type=jnp.float32)

            @pl.when(dist == 0)
            def _():
                total[part, :] = product

            @pl.when(dist > 0)
            def _():
                total[part, :] += product

    def at_distance(dist, part="all"):
        if cut == 0:
            if part in ("own", "cut"):
                return
            part = "all"
        lax.fori_loop(0, 2, lambda j, c: (multiply(j, dist, part), c)[1], 0)

    def relay(d, carry):
        for step, (o, q) in enumerate([(0, q) for q in range(CHUNKS)] + crossed):
            for k in range(2):
                from_z = z - d if k == 0 else z + d

                @pl.when((from_z >= 0) & (from_z < line))
                def _():
                    block = from_z * lanes + side(o)
                    index = block * CHUNKS + q
                    arrived(index)
                    along(k, chunk(index), index, send_zb.at[k, block] if o else send_z.at[k, from_z])
                    if q < last:
                        across(chunk(index), index, from_z)

            if step == CHUNKS // 3:
                @pl.when(d == 2)
                def _():
                    for source in far:
                        pltpu.make_async_copy(a_buf.at[source], a_buf.at[source], a_recv.at[source]).wait()
                        a_copy(a_buf.at[source], source, a_send_p.at[source], partner).start()

            if step == CHUNKS // 6:
                @pl.when(d == line - 1)
                def _():
                    at_distance(line - 3)

            for when, dist, part in ((CHUNKS // 2, line - 2, "own"), (CHUNKS - 2, line - 2, "cut"),
                                     (CHUNKS - 2, line - 2, "rest"), (CHUNKS - 1, line - 1, "own"),
                                     (CHUNKS - 1, line - 1, "cut")):
                if step == when:
                    @pl.when(d == line - 1)
                    def _():
                        at_distance(dist, part)

            if step == CHUNKS - 1:
                @pl.when(d == 2)
                def _():
                    for copy in mine:
                        copy.wait()
                    for x in range(half):
                        source = x * 2 + 1 - bc
                        pltpu.make_async_copy(a_buf.at[source], a_buf.at[source], a_recv.at[source]).wait()

                @pl.when((d >= 2) & (d < line - 1))
                def _():
                    at_distance(d - 2)
        return carry

    lax.fori_loop(1, line, relay, 0)
    at_distance(line - 1, "rest")

    def squares(t, c):
        v = total[pl.ds(pl.multiple_of(t * tile, tile), tile), :]
        return c + jnp.sum(v * v, axis=0, keepdims=True)

    stats[me] = lax.fori_loop(0, rows // tile, squares, jnp.zeros((1, total.shape[1]), jnp.float32))

    def share(o, target, slot):
        return pltpu.make_async_remote_copy(
            src_ref=stats.at[me], dst_ref=stats.at[me], send_sem=s_send.at[o], recv_sem=s_recv.at[slot],
            device_id=ga(target), device_id_type=MESH)

    for o in range(1, n_ga):
        share(o, lax.rem(me + o, n_ga), me).start()
    for o in range(1, n_ga):
        source = lax.rem(me + o, n_ga)
        pltpu.make_async_copy(stats.at[source], stats.at[source], s_recv.at[source]).wait()
    everything = stats[0]
    for g in range(1, n_ga):
        everything = everything + stats[g]
    rms = jnp.sqrt(everything / (rows * n_ga) + 1e-06)
    rms_out[...] = rms
    for o in range(1, n_ga):
        share(o, lax.rem(me + o, n_ga), me).wait_send()
    for o, target in enumerate(far):
        a_copy(coef, mb, a_send_x.at[o], target).wait_send()
    for x in range(half):
        a_copy(coef, x * 2 + bc, a_send_p.at[x * 2 + bc], partner).wait_send()

    def sent(count, sem):
        view = b_buf.at[pl.ds(0, count * piece)]
        pltpu.make_async_copy(view, view, sem).wait()

    for from_z in range(line):
        for k in range(2):
            @pl.when((z >= from_z) & (z < line - 1) if k == 0 else (z <= from_z) & (z > 0))
            def _():
                sent(CHUNKS, send_z.at[k, from_z])
                for o in range(1, lanes):
                    sent(CROSS, send_zb.at[k, from_z * lanes + side(o)])
        for o in range(1, lanes):
            @pl.when(z == from_z)
            def _():
                sent(CHUNKS, send_y.at[o - 1, from_z])

            @pl.when(z != from_z)
            def _():
                sent(last, send_y.at[o - 1, from_z])


PIECES = 12
GIVEN = 10


def edge_kernel(n_ga, n_ba, line, lent, coef, rot, total, rms_out, a_buf, c_buf, b_buf, f_buf, l_buf, stats,
                recv, send_z, send_zb, send_y, f_recv, f_send, f_cross, a_recv, a_send_x, a_send_p,
                c_recv, c_send, l_recv, l_send, s_recv, s_send, own):
    lanes = n_ga // line
    depth = rot.shape[0]
    rows, width = coef.shape
    kept = rot.shape[1] - lent
    piece = depth // PIECES
    given = rows // GIVEN
    last = PIECES - 1
    half = rows // 2
    me, mb = lax.axis_index("ga"), lax.axis_index("ba")
    z, w = me // lanes, lax.rem(me, lanes)
    v = 1 - w
    bx, bc = mb // 2, lax.rem(mb, 2)
    partner = mb + 1 - 2 * bc
    far = (1 - bx) * 2 + bc
    beyond = (1 - bx) * 2 + 1 - bc
    inside = lax.rem((z + 1) // 2, 2)
    upper = z // (line // 2)
    mate = z + 1 - 2 * lax.rem(z, 2)
    toward = z + 1 - 2 * upper
    skip = upper * (line - 1)
    sx, sc = skip // 2, lax.rem(skip, 2)
    crosses = bc + sc - 2 * bc * sc
    late = (1 - crosses) * (1 - bx - sx + 2 * bx * sx)
    entry = mb + late * (far - mb)

    def ga(i):
        return {"ga": i}

    def ba(i):
        return {"ba": i}

    def remote(src, dst, send, arrive, target):
        return pltpu.make_async_remote_copy(
            src_ref=src, dst_ref=dst, send_sem=send, recv_sem=arrive, device_id=target, device_id_type=MESH)

    def landed(ref, sem):
        pltpu.make_async_copy(ref, ref, sem).wait()

    barrier = pltpu.get_barrier_semaphore()
    def greet(device):
        pl.semaphore_signal(barrier, inc=1, device_id=device, device_id_type=MESH)

    @pl.when(z > 0)
    def _():
        greet(ga(me - lanes))

    @pl.when(z < line - 1)
    def _():
        greet(ga(me + lanes))

    greet(ga(z * lanes + v))
    greet(ba(far))
    greet(ba(partner))

    mine = [
        pltpu.make_async_copy(
            rot.at[:, pl.ds(lent, kept)], b_buf.at[pl.ds(pl.multiple_of(me * depth, depth), depth)], own.at[0]),
        pltpu.make_async_copy(
            rot.at[:, pl.ds(0, lent)], f_buf.at[pl.ds(pl.multiple_of(me * depth, depth), depth)], own.at[1]),
        pltpu.make_async_copy(coef, a_buf.at[mb], own.at[2]),
    ]
    ends = (line - 1 - z) // (line - 1) + z // (line - 1)
    pl.semaphore_wait(barrier, 2 - ends + 3)

    def chunk(index):
        return b_buf.at[pl.ds(pl.multiple_of(index * piece, piece), piece)]

    def arrived(index):
        landed(chunk(index), recv.at[index])

    def along(k, src, index, sem):
        @pl.when(z < line - 1 if k == 0 else z > 0)
        def _():
            remote(src, chunk(index), sem, recv.at[index], ga(me + lanes if k == 0 else me - lanes)).start()

    def across(src, index, from_z):
        remote(src, chunk(index), send_y.at[from_z], recv.at[index], ga(z * lanes + v)).start()

    def own_chunk(q):
        return rot.at[pl.ds(q * piece, piece), pl.ds(lent, kept)]

    def f_block(block):
        return f_buf.at[pl.ds(pl.multiple_of(block * depth, depth), depth)]

    def f_arrived(block):
        landed(f_block(block), f_recv.at[block])

    def f_along(src, block):
        remote(src, f_block(block), f_send.at[block], f_recv.at[block], ga(toward * lanes + w)).start()

    f_own = rot.at[:, pl.ds(0, lent)]
    f_over = remote(f_own, f_block(me), f_cross.at[0], f_recv.at[me], ga(z * lanes + v))
    f_over.start()
    across(own_chunk(last), me * PIECES + last, z)
    f_along(f_own, me)
    for q in range(PIECES):
        for k in range(2):
            along(k, own_chunk(q), me * PIECES + q, send_z.at[k, z])
        if q < last:
            across(own_chunk(q), me * PIECES + q, z)

    def a_copy(src, index, sem, target):
        return remote(src, a_buf.at[index], sem, a_recv.at[index], ba(target))

    a_copy(coef, mb, a_send_x.at[0], far).start()
    a_copy(coef, mb, a_send_p.at[0], partner).start()
    for copy in mine:
        copy.start()

    total[...] = jnp.zeros_like(total)
    side = z * lanes + v
    f_arrived(side)
    f_along(f_block(side), side)
    arrived(side * PIECES + last)
    for k in range(2):
        along(k, chunk(side * PIECES + last), side * PIECES + last, send_zb.at[k, side])

    def strip(r):
        return pl.ds(pl.multiple_of(r * given, given), given)

    def c_at(block, r):
        return c_buf.at[block - 1 + upper, strip(r)]

    def c_copy(src, block, r, sem, target):
        return remote(src, c_at(block, r), sem, c_recv.at[block, r], target)

    def lend(source):
        @pl.loop(0, GIVEN)
        def _(r):
            c_copy(source.at[strip(r)], entry, r, c_send.at[0], ga(mate * lanes + w)).start()

    @pl.when((inside == 0) & (late == 0))
    def _():
        lend(coef)

    @pl.when(inside == 1)
    def _():
        f_arrived(mate * lanes + w)
        f_along(f_block(mate * lanes + w), mate * lanes + w)

    def pass_entry(r):
        landed(c_at(entry, r), c_recv.at[entry, r])

        @pl.when(crosses == 1)
        def _():
            c_copy(c_at(entry, r), entry, r, c_send.at[1], ba(far)).start()

        c_copy(c_at(entry, r), entry, r, c_send.at[2], ba(partner)).start()

    def pass_far(r):
        @pl.when(crosses == 1)
        def _():
            landed(c_at(far, r), c_recv.at[far, r])
            c_copy(c_at(far, r), far, r, c_send.at[3], ba(partner)).start()

    def ready():
        for copy in mine:
            copy.wait()
        for source in (partner, beyond):
            landed(a_buf.at[source], a_recv.at[source])

    def order(i):
        j, lane = i // lanes, lax.rem(i, lanes)
        near = j + inside * (1 - j // 2) * (1 - 2 * lax.rem(j, 2))
        from_z = near + upper * (line - 1 - 2 * near)
        return from_z * lanes + w + lane * (1 - 2 * w), lane

    def panel(begin, size):
        at, column = begin // width, pl.multiple_of(lax.rem(begin, width), 128)

        @pl.loop(0, 2)
        def _(t):
            part = pl.ds(pl.multiple_of(t * half, half), half)
            total[part, pl.ds(lent, kept)] += jnp.dot(
                a_buf[at, part, pl.ds(column, size)],
                b_buf[pl.ds(pl.multiple_of(begin, 128), size), :],
                preferred_element_type=jnp.float32)

    def crossing(block, begin, end):
        @pl.loop(begin, end)
        def _(q):
            arrived(block * PIECES + q)

    def whole(i):
        block, lane = order(i)

        @pl.when(lane == 1)
        def _():
            crossing(block, 0, last)

        panel(block * depth, depth)

    steps = PIECES + 1

    @pl.loop(0, (line - 1) * steps)
    def _(t):
        d, step = 1 + t // steps, lax.rem(t, steps)
        crossed = step // PIECES
        q = step - crossed

        @pl.when((inside == 1) & (d == 1) & (step == last))
        def _():
            f_arrived(mate * lanes + v)
            f_along(f_block(mate * lanes + v), mate * lanes + v)

        for k in range(2):
            from_z = z - d if k == 0 else z + d

            @pl.when((from_z >= 0) & (from_z < line))
            def _():
                @pl.when(crossed == 0)
                def _():
                    index = (from_z * lanes + w) * PIECES + q
                    arrived(index)
                    along(k, chunk(index), index, send_z.at[k, from_z])

                    @pl.when(q < last)
                    def _():
                        across(chunk(index), index, from_z)

                @pl.when(crossed == 1)
                def _():
                    block = from_z * lanes + v
                    index = block * PIECES + q
                    arrived(index)
                    along(k, chunk(index), index, send_zb.at[k, block])

        @pl.when((d == 2) & (step == inside * 4 + (1 - inside) * PIECES))
        def _():
            landed(a_buf.at[far], a_recv.at[far])
            a_copy(a_buf.at[far], far, a_send_p.at[1], partner).start()

            @pl.when((inside == 0) & (late == 1))
            def _():
                lend(a_buf.at[far])

        @pl.when((inside == 1) & (d == 2) & (lax.rem(step, 2) == 1))
        def _():
            r = step // 2

            @pl.when(late == 0)
            def _():
                pass_entry(r)

            @pl.when(r >= 3)
            def _():
                pass_far(r - 3)

        turn = step - inside * 6 - (1 - inside) * 2

        @pl.when((d == 3 - inside) & (turn >= 0) & (turn < 8) & (lax.rem(turn + 8, 2) == 0))
        def _():
            n = turn // 2

            @pl.when(n == 0)
            def _():
                ready()

            whole(n + n // 3)

    def lent_product(source, part, begin, count):
        product = jnp.dot(
            source[0, part, :], f_buf[pl.ds(begin, width), :], preferred_element_type=jnp.float32)
        for s in range(1, count):
            product += jnp.dot(
                source[s, part, :], f_buf[pl.ds(begin + s * width, width), :], preferred_element_type=jnp.float32)
        return product

    @pl.when(inside == 1)
    def _():
        for from_z in (toward, toward + 1 - 2 * lax.rem(toward, 2)):
            for lane in range(lanes):
                f_arrived(from_z * lanes + lane)

        @pl.when(late == 1)
        def _():
            pass_entry(0)
            pass_entry(1)

    @pl.loop(0, GIVEN)
    def _(r):
        @pl.when(inside == 1)
        def _():
            @pl.when(late == 1)
            def _():
                @pl.when(r + 2 < GIVEN)
                def _():
                    pass_entry(r + 2)

            @pl.when(late == 0)
            def _():
                for when, which in ((0, 6), (1, 7), (4, 8), (6, 9)):
                    @pl.when(r == when)
                    def _():
                        pass_entry(which)

            @pl.when(r < 4)
            def _():
                pass_far(3 + r)

            @pl.when(r >= 7)
            def _():
                pass_far(r)

            @pl.when(crosses == 1)
            def _():
                given_block = (1 - sx) * 2 + sc
                landed(c_at(given_block, r), c_recv.at[given_block, r])

            @pl.when(crosses == 0)
            def _():
                for source in (partner, beyond):
                    landed(c_at(source, r), c_recv.at[source, r])

            l_buf[strip(r), :] = lent_product(
                c_buf, strip(r), pl.multiple_of((1 - upper) * width, width), n_ba - 1)
            remote(l_buf.at[strip(r)], l_buf.at[strip(r)], l_send.at[0], l_recv.at[r], ga(mate * lanes + w)).start()

        @pl.when(r < 3)
        def _():
            whole(6 - r * 3 + r // 2 * 5)

        @pl.when((r == 3) | (r == 4))
        def _():
            part = pl.ds(pl.multiple_of((r - 3) * half, half), half)

            @pl.when(inside == 1)
            def _():
                total[part, pl.ds(0, lent)] = lent_product(a_buf, part, 0, n_ba)

            @pl.when(inside == 0)
            def _():
                total[part, pl.ds(0, lent)] = jnp.dot(
                    a_buf[skip, part, :], f_buf[pl.ds(pl.multiple_of(skip * width, width), width), :],
                    preferred_element_type=jnp.float32)

    final, _ = order(7)
    cut = last * piece // 256 * 256
    crossing(final, 0, cut // piece)
    panel(final * depth, cut)

    @pl.when(inside == 0)
    def _():
        @pl.loop(0, GIVEN)
        def _(r):
            landed(l_buf.at[strip(r)], l_recv.at[r])
            total[strip(r), pl.ds(0, lent)] += l_buf[strip(r), :]

    crossing(final, cut // piece, last)
    panel(final * depth + cut, depth - cut)

    v_all = total[...]
    stats[me] = jnp.sum(v_all * v_all, axis=0, keepdims=True)

    def share(o, target, slot):
        return remote(stats.at[me], stats.at[me], s_send.at[o], s_recv.at[slot], ga(target))

    for o in range(1, n_ga):
        share(o, lax.rem(me + o, n_ga), me).start()

    a_copy(coef, mb, a_send_x.at[0], far).wait_send()
    for i in range(2):
        a_copy(coef, mb, a_send_p.at[i], partner).wait_send()

    def sent(count, sem):
        landed(b_buf.at[pl.ds(0, count * piece)], sem)

    f_over.wait_send()
    for lane in range(lanes):
        block = z * lanes + lane
        landed(f_block(block), f_send.at[block])

    @pl.when(inside == 0)
    def _():
        landed(c_buf.at[0], c_send.at[0])

    @pl.when(inside == 1)
    def _():
        for lane in range(lanes):
            block = mate * lanes + lane
            landed(f_block(block), f_send.at[block])
        landed(c_buf.at[0], c_send.at[2])
        landed(l_buf, l_send.at[0])

        @pl.when(crosses == 1)
        def _():
            landed(c_buf.at[0], c_send.at[1])
            landed(c_buf.at[0], c_send.at[3])

    for from_z in range(line):
        for k in range(2):
            @pl.when((z >= from_z) & (z < line - 1) if k == 0 else (z <= from_z) & (z > 0))
            def _():
                sent(PIECES, send_z.at[k, from_z])
                sent(1, send_zb.at[k, from_z * lanes + v])

        @pl.when(z == from_z)
        def _():
            sent(PIECES, send_y.at[from_z])

        @pl.when(z != from_z)
        def _():
            sent(last, send_y.at[from_z])

    for o in range(1, n_ga):
        source = lax.rem(me + o, n_ga)
        landed(stats.at[source], s_recv.at[source])
    everything = stats[0]
    for g in range(1, n_ga):
        everything = everything + stats[g]
    rms_out[...] = jnp.sqrt(everything / (rows * n_ga) + 1e-06)
    for o in range(1, n_ga):
        share(o, lax.rem(me + o, n_ga), me).wait_send()


def solution(mesh):
    n_ga, n_ba = mesh.shape["ga"], mesh.shape["ba"]
    line = 2 ** math.ceil(math.log2(n_ga) / 2)
    lanes = n_ga // line

    def edges(rows, width, depth, columns):
        dma = pltpu.SemaphoreType.DMA
        lent = columns // LENT // 128 * 128
        return functools.partial(edge_kernel, n_ga, n_ba, line, lent), [
            pltpu.VMEM((n_ba, rows, width), jnp.bfloat16),
            pltpu.VMEM((n_ba - 1, rows, width), jnp.bfloat16),
            pltpu.VMEM((n_ga * depth, columns - lent), jnp.bfloat16),
            pltpu.VMEM((n_ga * depth, lent), jnp.bfloat16),
            pltpu.VMEM((rows, lent), jnp.float32),
            pltpu.VMEM((n_ga, 1, columns), jnp.float32),
            dma((n_ga * PIECES,)),
            dma((2, line)),
            dma((2, n_ga)),
            dma((line,)),
            dma((n_ga,)),
            dma((n_ga,)),
            dma((1,)),
            dma((n_ba,)),
            dma((1,)),
            dma((2,)),
            dma((n_ba, GIVEN)),
            dma((4,)),
            dma((GIVEN,)),
            dma((1,)),
            dma((n_ga,)),
            dma((n_ga,)),
            dma((3,)),
        ], 56 * 2**20

    def plain(rows, width, depth, columns):
        dma = pltpu.SemaphoreType.DMA
        return functools.partial(kernel, n_ga, n_ba, line), [
            pltpu.VMEM((n_ba, rows, width), jnp.bfloat16),
            pltpu.VMEM((n_ga * depth, columns), jnp.bfloat16),
            pltpu.VMEM((n_ga, 1, columns), jnp.float32),
            dma((n_ga * CHUNKS,)),
            dma((2, line)),
            dma((2, n_ga)),
            dma((lanes - 1, line)),
            dma((n_ba,)),
            dma((n_ba // 2 - 1,)),
            dma((n_ba,)),
            dma((n_ga,)),
            dma((n_ga,)),
            dma((2,)),
        ], 48 * 2**20

    def body(coef, rot):
        rows, width = coef.shape
        depth, columns = rot.shape
        build = edges if (line, lanes, n_ba) == (4, 2, 4) else plain
        run, scratch, limit = build(rows, width, depth, columns)
        rotated, rms = pl.pallas_call(
            run,
            out_shape=(pltpu.VMEM((rows, columns), jnp.float32),
                       pltpu.VMEM((1, columns), jnp.float32)),
            in_specs=[pl.BlockSpec(memory_space=pltpu.HBM)] * 2,
            out_specs=(pl.BlockSpec(memory_space=pltpu.VMEM),) * 2,
            scratch_shapes=scratch,
            compiler_params=pltpu.CompilerParams(
                collective_id=0, has_side_effects=True, vmem_limit_bytes=limit),
        )(*(pltpu.with_memory_space_constraint(x, pltpu.HBM) for x in (coef, rot)))
        return (rotated * (1.0 / rms)).astype(jnp.bfloat16), rms.reshape(columns)

    return jax.shard_map(body, mesh=mesh, in_specs=(P("ga", "ba"), P("ga", "ba")),
                         out_specs=(P("ga", "ba"), P("ba")), check_vma=False)
```

```python
import functools
import math

import jax
import jax.numpy as jnp
from jax import lax
from jax.experimental import pallas as pl
from jax.experimental.pallas import tpu as pltpu
from jax.sharding import PartitionSpec as P

MESH = pl.DeviceIdType.MESH
CHUNKS = 6
CROSS = 1
LENT = 6


def kernel(n_ga, n_ba, line, coef, rot, total, rms_out, a_buf, b_buf, stats,
           recv, send_z, send_zb, send_y, a_recv, a_send_x, a_send_p, s_recv, s_send, own):
    lanes = n_ga // line
    depth = rot.shape[0]
    rows, width = coef.shape
    piece = depth // CHUNKS
    span = lanes * depth
    me, mb = lax.axis_index("ga"), lax.axis_index("ba")
    z, w = me // lanes, lax.rem(me, lanes)
    bx, bc = mb // 2, lax.rem(mb, 2)
    half = n_ba // 2

    def ga(i):
        return {"ga": i}

    def side(o):
        return lax.rem(w + o, lanes)

    def chunk(index):
        return b_buf.at[pl.ds(pl.multiple_of(index * piece, piece), piece)]

    partner = mb + 1 - 2 * bc
    far = [lax.rem(bx + o, half) * 2 + bc for o in range(1, half)]

    barrier = pltpu.get_barrier_semaphore()
    def greet(device):
        pl.semaphore_signal(barrier, inc=1, device_id=device, device_id_type=MESH)

    @pl.when(z > 0)
    def _():
        greet(ga(me - lanes))

    @pl.when(z < line - 1)
    def _():
        greet(ga(me + lanes))

    for o in range(1, lanes):
        greet(ga(z * lanes + side(o)))
    for target in [*far, partner]:
        greet({"ba": target})

    mine = [
        pltpu.make_async_copy(rot, b_buf.at[pl.ds(pl.multiple_of(me * depth, depth), depth)], own.at[0]),
        pltpu.make_async_copy(coef, a_buf.at[mb], own.at[1]),
    ]
    ends = (line - 1 - z) // (line - 1) + z // (line - 1)
    pl.semaphore_wait(barrier, 2 - ends + lanes - 1 + len(far) + 1)

    def remote(src, index, sem, target):
        return pltpu.make_async_remote_copy(
            src_ref=src, dst_ref=chunk(index), send_sem=sem, recv_sem=recv.at[index],
            device_id=ga(target), device_id_type=MESH)

    def arrived(index):
        pltpu.make_async_copy(chunk(index), chunk(index), recv.at[index]).wait()

    def along(k, src, index, sem):
        @pl.when(z < line - 1 if k == 0 else z > 0)
        def _():
            remote(src, index, sem, me + lanes if k == 0 else me - lanes).start()

    def across(src, index, from_z):
        for o in range(1, lanes):
            remote(src, index, send_y.at[o - 1, from_z], z * lanes + side(o)).start()

    def own_chunk(q):
        return rot.at[pl.ds(q * piece, piece)]

    last = CHUNKS - CROSS
    crossed = [(o, q) for q in range(last, CHUNKS) for o in range(1, lanes)]
    for q in range(last, CHUNKS):
        across(own_chunk(q), me * CHUNKS + q, z)
    for q in range(CHUNKS):
        for k in range(2):
            along(k, own_chunk(q), me * CHUNKS + q, send_z.at[k, z])
        if q < last:
            across(own_chunk(q), me * CHUNKS + q, z)

    def a_copy(src, index, sem, target):
        return pltpu.make_async_remote_copy(
            src_ref=src, dst_ref=a_buf.at[index], send_sem=sem, recv_sem=a_recv.at[index],
            device_id={"ba": target}, device_id_type=MESH)

    for o, target in enumerate(far):
        a_copy(coef, mb, a_send_x.at[o], target).start()
    a_copy(coef, mb, a_send_p.at[mb], partner).start()
    for copy in mine:
        copy.start()

    for o, q in crossed:
        index = (z * lanes + side(o)) * CHUNKS + q
        arrived(index)
        for k in range(2):
            along(k, chunk(index), index, send_zb.at[k, z * lanes + side(o)])

    tile = math.gcd(rows, 1280)

    def multiply(j, dist, part):
        from_z = z - dist + 2 * dist * j

        @pl.when((from_z >= 0) & (from_z < line) & ((dist > 0) | (j == 0)))
        def _():
            if part == "all":
                for o in range(1, lanes):
                    for q in range(last):
                        arrived((from_z * lanes + side(o)) * CHUNKS + q)
                panel(from_z * span, span, dist)
                return
            if part == "own":
                panel((from_z * lanes + w) * depth, depth, dist)
                return
            for o in range(1, lanes):
                block = from_z * lanes + side(o)
                for q in range(cut) if part == "cut" else range(cut, last):
                    arrived(block * CHUNKS + q)
                if part == "cut":
                    panel(block * depth, cut * piece, dist)
                else:
                    panel(block * depth + cut * piece, depth - cut * piece, dist)

    cut = max(q for q in range(last) if q * piece % 128 == 0) if depth % 128 == 0 else 0

    def panel(begin, size, dist):
        at, column = begin // width, pl.multiple_of(lax.rem(begin, width), 128)

        @pl.loop(0, rows // tile)
        def _(t):
            part = pl.ds(pl.multiple_of(t * tile, tile), tile)
            product = jnp.dot(
                a_buf[at, part, pl.ds(column, size)],
                b_buf[pl.ds(pl.multiple_of(begin, 128), size), :],
                preferred_element_type=jnp.float32)

            @pl.when(dist == 0)
            def _():
                total[part, :] = product

            @pl.when(dist > 0)
            def _():
                total[part, :] += product

    def at_distance(dist, part="all"):
        if cut == 0:
            if part in ("own", "cut"):
                return
            part = "all"
        lax.fori_loop(0, 2, lambda j, c: (multiply(j, dist, part), c)[1], 0)

    def relay(d, carry):
        for step, (o, q) in enumerate([(0, q) for q in range(CHUNKS)] + crossed):
            for k in range(2):
                from_z = z - d if k == 0 else z + d

                @pl.when((from_z >= 0) & (from_z < line))
                def _():
                    block = from_z * lanes + side(o)
                    index = block * CHUNKS + q
                    arrived(index)
                    along(k, chunk(index), index, send_zb.at[k, block] if o else send_z.at[k, from_z])
                    if q < last:
                        across(chunk(index), index, from_z)

            if step == CHUNKS // 3:
                @pl.when(d == 2)
                def _():
                    for source in far:
                        pltpu.make_async_copy(a_buf.at[source], a_buf.at[source], a_recv.at[source]).wait()
                        a_copy(a_buf.at[source], source, a_send_p.at[source], partner).start()

            if step == CHUNKS // 6:
                @pl.when(d == line - 1)
                def _():
                    at_distance(line - 3)

            for when, dist, part in ((CHUNKS // 2, line - 2, "own"), (CHUNKS - 2, line - 2, "cut"),
                                     (CHUNKS - 2, line - 2, "rest"), (CHUNKS - 1, line - 1, "own"),
                                     (CHUNKS - 1, line - 1, "cut")):
                if step == when:
                    @pl.when(d == line - 1)
                    def _():
                        at_distance(dist, part)

            if step == CHUNKS - 1:
                @pl.when(d == 2)
                def _():
                    for copy in mine:
                        copy.wait()
                    for x in range(half):
                        source = x * 2 + 1 - bc
                        pltpu.make_async_copy(a_buf.at[source], a_buf.at[source], a_recv.at[source]).wait()

                @pl.when((d >= 2) & (d < line - 1))
                def _():
                    at_distance(d - 2)
        return carry

    lax.fori_loop(1, line, relay, 0)
    at_distance(line - 1, "rest")

    def squares(t, c):
        v = total[pl.ds(pl.multiple_of(t * tile, tile), tile), :]
        return c + jnp.sum(v * v, axis=0, keepdims=True)

    stats[me] = lax.fori_loop(0, rows // tile, squares, jnp.zeros((1, total.shape[1]), jnp.float32))

    def share(o, target, slot):
        return pltpu.make_async_remote_copy(
            src_ref=stats.at[me], dst_ref=stats.at[me], send_sem=s_send.at[o], recv_sem=s_recv.at[slot],
            device_id=ga(target), device_id_type=MESH)

    for o in range(1, n_ga):
        share(o, lax.rem(me + o, n_ga), me).start()
    for o in range(1, n_ga):
        source = lax.rem(me + o, n_ga)
        pltpu.make_async_copy(stats.at[source], stats.at[source], s_recv.at[source]).wait()
    everything = stats[0]
    for g in range(1, n_ga):
        everything = everything + stats[g]
    rms = jnp.sqrt(everything / (rows * n_ga) + 1e-06)
    rms_out[...] = rms
    for o in range(1, n_ga):
        share(o, lax.rem(me + o, n_ga), me).wait_send()
    for o, target in enumerate(far):
        a_copy(coef, mb, a_send_x.at[o], target).wait_send()
    for x in range(half):
        a_copy(coef, x * 2 + bc, a_send_p.at[x * 2 + bc], partner).wait_send()

    def sent(count, sem):
        view = b_buf.at[pl.ds(0, count * piece)]
        pltpu.make_async_copy(view, view, sem).wait()

    for from_z in range(line):
        for k in range(2):
            @pl.when((z >= from_z) & (z < line - 1) if k == 0 else (z <= from_z) & (z > 0))
            def _():
                sent(CHUNKS, send_z.at[k, from_z])
                for o in range(1, lanes):
                    sent(CROSS, send_zb.at[k, from_z * lanes + side(o)])
        for o in range(1, lanes):
            @pl.when(z == from_z)
            def _():
                sent(CHUNKS, send_y.at[o - 1, from_z])

            @pl.when(z != from_z)
            def _():
                sent(last, send_y.at[o - 1, from_z])


PIECES = 12
GIVEN = 10


def edge_kernel(n_ga, n_ba, line, lent, coef, rot, out, rms_out, total, a_buf, c_buf, b_buf, f_buf, l_buf, stats,
                recv, recv_y, recv_x, send_z, send_y, f_recv, f_send, a_recv, a_send,
                c_recv, c_send, l_recv, l_send, s_recv, s_send, own):
    lanes = n_ga // line
    depth = rot.shape[0]
    rows, width = coef.shape
    kept = rot.shape[1] - lent
    piece = depth // PIECES
    given = rows // GIVEN
    last = PIECES - 1
    half = rows // 2
    me, mb = lax.axis_index("ga"), lax.axis_index("ba")
    z, w = me // lanes, lax.rem(me, lanes)
    v = 1 - w
    bx, bc = mb // 2, lax.rem(mb, 2)
    partner = mb + 1 - 2 * bc
    far = (1 - bx) * 2 + bc
    beyond = (1 - bx) * 2 + 1 - bc
    inside = lax.rem((z + 1) // 2, 2)
    upper = z // (line // 2)
    mate = z + 1 - 2 * lax.rem(z, 2)
    toward = z + 1 - 2 * upper
    skip = upper * (line - 1)
    sx, sc = skip // 2, lax.rem(skip, 2)
    crosses = bc + sc - 2 * bc * sc
    late = (1 - crosses) * (1 - bx - sx + 2 * bx * sx)
    entry = mb + late * (far - mb)

    def ga(i):
        return {"ga": i}

    def ba(i):
        return {"ba": i}

    def remote(src, dst, send, arrive, target):
        return pltpu.make_async_remote_copy(
            src_ref=src, dst_ref=dst, send_sem=send, recv_sem=arrive, device_id=target, device_id_type=MESH)

    def landed(ref, sem):
        pltpu.make_async_copy(ref, ref, sem).wait()

    barrier = pltpu.get_barrier_semaphore()
    def greet(device):
        pl.semaphore_signal(barrier, inc=1, device_id=device, device_id_type=MESH)

    @pl.when(z > 0)
    def _():
        greet(ga(me - lanes))

    @pl.when(z < line - 1)
    def _():
        greet(ga(me + lanes))

    greet(ga(z * lanes + v))
    greet(ba(far))
    greet(ba(partner))

    mine = [
        pltpu.make_async_copy(
            rot.at[:, pl.ds(lent, kept)], b_buf.at[pl.ds(pl.multiple_of(me * depth, depth), depth)], own.at[0]),
        pltpu.make_async_copy(
            rot.at[:, pl.ds(0, lent)], f_buf.at[pl.ds(pl.multiple_of(me * depth, depth), depth)], own.at[1]),
        pltpu.make_async_copy(coef, a_buf.at[mb], own.at[2]),
    ]
    ends = (line - 1 - z) // (line - 1) + z // (line - 1)
    pl.semaphore_wait(barrier, 2 - ends + 3)

    def chunk(index):
        return b_buf.at[pl.ds(pl.multiple_of(index * piece, piece), piece)]

    cut = last * piece // 256 * 256
    early = cut // piece

    def along(k, src, index, arrive):
        @pl.when(z < line - 1 if k == 0 else z > 0)
        def _():
            remote(src, chunk(index), send_z.at[k], arrive, ga(me + lanes if k == 0 else me - lanes)).start()

    def across(src, from_z, q):
        index = (from_z * lanes + w) * PIECES + q
        slot = from_z * 2 + q // early
        remote(src, chunk(index), send_y.at[0], recv_y.at[slot], ga(z * lanes + v)).start()

    def crossed_over(block, part):
        begin, count = (0, early) if part == 0 else (early, last - early)
        view = b_buf.at[pl.ds(pl.multiple_of(block * depth + begin * piece, piece), count * piece)]
        landed(view, recv_y.at[block // lanes * 2 + part])

    def own_chunk(q):
        return rot.at[pl.ds(q * piece, piece), pl.ds(lent, kept)]

    def f_block(block):
        return f_buf.at[pl.ds(pl.multiple_of(block * depth, depth), depth)]

    def f_arrived(block, slot):
        landed(f_block(block), f_recv.at[slot])

    def f_along(src, block, slot):
        remote(src, f_block(block), f_send.at[0], f_recv.at[slot + inside * (3 - slot)], ga(toward * lanes + w)).start()

    f_own = rot.at[:, pl.ds(0, lent)]
    f_over = remote(f_own, f_block(me), f_send.at[1], f_recv.at[0], ga(z * lanes + v))
    f_over.start()
    over = remote(own_chunk(last), chunk(me * PIECES + last), send_y.at[1], recv_x.at[z], ga(z * lanes + v))
    over.start()
    f_along(f_own, me, 1)
    for q in range(PIECES):
        for k in range(2):
            along(k, own_chunk(q), me * PIECES + q, recv.at[z * PIECES + q])
        if q < last:
            across(own_chunk(q), z, q)

    def a_copy(src, index, sem, target):
        return remote(src, a_buf.at[index], sem, a_recv.at[index], ba(target))

    a_copy(coef, mb, a_send.at[0], far).start()
    a_copy(coef, mb, a_send.at[1], partner).start()
    for copy in mine:
        copy.start()

    total[...] = jnp.zeros_like(total)
    side = z * lanes + v
    f_arrived(side, 0)
    f_along(f_block(side), side, 2)
    landed(chunk(side * PIECES + last), recv_x.at[z])
    for k in range(2):
        along(k, chunk(side * PIECES + last), side * PIECES + last, recv_x.at[z])

    def strip(r):
        return pl.ds(pl.multiple_of(r * given, given), given)

    def c_at(block, r):
        return c_buf.at[block - 1 + upper, strip(r)]

    def c_copy(src, block, r, kind, sem, target):
        return remote(src, c_at(block, r), c_send.at[sem], c_recv.at[kind * GIVEN + r], target)

    def lend(source):
        @pl.loop(0, GIVEN)
        def _(r):
            c_copy(source.at[strip(r)], entry, r, 0, 0, ga(mate * lanes + w)).start()

    @pl.when((inside == 0) & (late == 0))
    def _():
        lend(coef)

    @pl.when(inside == 1)
    def _():
        f_arrived(mate * lanes + w, 1)
        f_along(f_block(mate * lanes + w), mate * lanes + w, 3)

    def pass_entry(r):
        landed(c_at(entry, r), c_recv.at[r])

        @pl.when(crosses == 1)
        def _():
            c_copy(c_at(entry, r), entry, r, 1, 1, ba(far)).start()

        c_copy(c_at(entry, r), entry, r, 2, 2, ba(partner)).start()

    def pass_far(r):
        @pl.when(crosses == 1)
        def _():
            landed(c_at(far, r), c_recv.at[GIVEN + r])
            c_copy(c_at(far, r), far, r, 2, 2, ba(partner)).start()

    def ready():
        for copy in mine:
            copy.wait()
        for source in (partner, beyond):
            landed(a_buf.at[source], a_recv.at[source])

    def order(i):
        j, lane = i // lanes, lax.rem(i, lanes)
        near = j + inside * (1 - j // 2) * (1 - 2 * lax.rem(j, 2))
        from_z = near + upper * (line - 1 - 2 * near)
        return from_z * lanes + w + lane * (1 - 2 * w), lane

    def panel(begin, size):
        at, column = begin // width, pl.multiple_of(lax.rem(begin, width), 128)

        @pl.loop(0, 2)
        def _(t):
            part = pl.ds(pl.multiple_of(t * half, half), half)
            total[part, pl.ds(lent, kept)] += jnp.dot(
                a_buf[at, part, pl.ds(column, size)],
                b_buf[pl.ds(pl.multiple_of(begin, 128), size), :],
                preferred_element_type=jnp.float32)

    def whole(i):
        block, lane = order(i)

        @pl.when(lane == 1)
        def _():
            crossed_over(block, 0)
            crossed_over(block, 1)

        panel(block * depth, depth)

    steps = PIECES + 1

    @pl.loop(0, (line - 1) * steps)
    def _(t):
        d, step = 1 + t // steps, lax.rem(t, steps)
        crossed = step // PIECES
        q = step - crossed

        @pl.when((inside == 1) & (d == 1) & (step == last))
        def _():
            f_arrived(mate * lanes + v, 2)
            f_along(f_block(mate * lanes + v), mate * lanes + v, 3)

        for k in range(2):
            from_z = z - d if k == 0 else z + d

            @pl.when((from_z >= 0) & (from_z < line))
            def _():
                @pl.when(crossed == 0)
                def _():
                    index = (from_z * lanes + w) * PIECES + q
                    sem = recv.at[from_z * PIECES + q]
                    landed(chunk(index), sem)
                    along(k, chunk(index), index, sem)

                    @pl.when(q < last)
                    def _():
                        across(chunk(index), from_z, q)

                @pl.when(crossed == 1)
                def _():
                    index = (from_z * lanes + v) * PIECES + last
                    landed(chunk(index), recv_x.at[from_z])
                    along(k, chunk(index), index, recv_x.at[from_z])

        @pl.when((d == 2) & (step == inside * 4 + (1 - inside) * PIECES))
        def _():
            landed(a_buf.at[far], a_recv.at[far])
            a_copy(a_buf.at[far], far, a_send.at[1], partner).start()

            @pl.when((inside == 0) & (late == 1))
            def _():
                lend(a_buf.at[far])

        @pl.when((inside == 1) & (d == 2) & (lax.rem(step, 2) == 1))
        def _():
            r = step // 2

            @pl.when(late == 0)
            def _():
                pass_entry(r)

            @pl.when(r >= 3)
            def _():
                pass_far(r - 3)

        turn = step - inside * 6 - (1 - inside) * 2

        @pl.when((d == 3 - inside) & (turn >= 0) & (turn < 8) & (lax.rem(turn + 8, 2) == 0))
        def _():
            n = turn // 2

            @pl.when(n == 0)
            def _():
                ready()

            whole(n + n // 3)

    def lent_product(source, part, begin, count):
        product = jnp.dot(
            source[0, part, :], f_buf[pl.ds(begin, width), :], preferred_element_type=jnp.float32)
        for s in range(1, count):
            product += jnp.dot(
                source[s, part, :], f_buf[pl.ds(begin + s * width, width), :], preferred_element_type=jnp.float32)
        return product

    @pl.when(inside == 1)
    def _():
        landed(f_buf.at[pl.ds(0, 2 * lanes * depth)], f_recv.at[3])

        @pl.when(late == 1)
        def _():
            pass_entry(0)
            pass_entry(1)

    @pl.loop(0, GIVEN)
    def _(r):
        @pl.when(inside == 1)
        def _():
            @pl.when(late == 1)
            def _():
                @pl.when(r + 2 < GIVEN)
                def _():
                    pass_entry(r + 2)

            @pl.when(late == 0)
            def _():
                for when, which in ((0, 6), (1, 7), (4, 8), (6, 9)):
                    @pl.when(r == when)
                    def _():
                        pass_entry(which)

            @pl.when(r < 4)
            def _():
                pass_far(3 + r)

            @pl.when(r >= 7)
            def _():
                pass_far(r)

            @pl.when(crosses == 1)
            def _():
                landed(c_at((1 - sx) * 2 + sc, r), c_recv.at[2 * GIVEN + r])

            @pl.when(crosses == 0)
            def _():
                landed(c_buf.at[pl.ds(0, 2), strip(r)], c_recv.at[2 * GIVEN + r])

            l_buf[strip(r), :] = lent_product(
                c_buf, strip(r), pl.multiple_of((1 - upper) * width, width), n_ba - 1)
            remote(l_buf.at[strip(r)], l_buf.at[strip(r)], l_send.at[0], l_recv.at[0], ga(mate * lanes + w)).start()

        @pl.when(r < 3)
        def _():
            whole(6 - r * 3 + r // 2 * 5)

        @pl.when((r == 3) | (r == 4))
        def _():
            part = pl.ds(pl.multiple_of((r - 3) * half, half), half)

            @pl.when(inside == 1)
            def _():
                total[part, pl.ds(0, lent)] = lent_product(a_buf, part, 0, n_ba)

            @pl.when(inside == 0)
            def _():
                total[part, pl.ds(0, lent)] = jnp.dot(
                    a_buf[skip, part, :], f_buf[pl.ds(pl.multiple_of(skip * width, width), width), :],
                    preferred_element_type=jnp.float32)

    final, _ = order(7)
    crossed_over(final, 0)
    panel(final * depth, cut)

    @pl.when(inside == 0)
    def _():
        landed(l_buf, l_recv.at[0])
        total[:, pl.ds(0, lent)] += l_buf[...]

    lent_part = total[:, pl.ds(0, lent)]
    stats[me, :, pl.ds(0, lent)] = jnp.sum(lent_part * lent_part, axis=0, keepdims=True)
    crossed_over(final, 1)
    begin = final * depth + cut
    at, column = begin // width, pl.multiple_of(lax.rem(begin, width), 128)

    def finish(t, squares):
        part = pl.ds(pl.multiple_of(t * half, half), half)
        done = total[part, pl.ds(lent, kept)] + jnp.dot(
            a_buf[at, part, pl.ds(column, depth - cut)],
            b_buf[pl.ds(pl.multiple_of(begin, 128), depth - cut), :],
            preferred_element_type=jnp.float32)
        total[part, pl.ds(lent, kept)] = done
        return squares + jnp.sum(done * done, axis=0, keepdims=True)

    stats[me, :, pl.ds(lent, kept)] = lax.fori_loop(0, 2, finish, jnp.zeros((1, kept), jnp.float32))

    def share(target):
        return remote(stats.at[me], stats.at[me], s_send.at[0], s_recv.at[0], ga(target))

    planes = (line - 1 - z, lax.rem(z + line // 2, line), mate)
    others = [plane * lanes + lane for plane in planes for lane in (v, w)] + [z * lanes + v]
    for target in others:
        share(target).start()

    def sent(count, sem):
        landed(b_buf.at[pl.ds(0, count * piece)], sem)

    landed(a_buf.at[0], a_send.at[0])
    landed(a_buf.at[pl.ds(0, 2)], a_send.at[1])
    f_over.wait_send()
    over.wait_send()

    @pl.when(inside == 0)
    def _():
        landed(f_buf.at[pl.ds(0, lanes * depth)], f_send.at[0])
        landed(c_buf.at[0], c_send.at[0])

    @pl.when(inside == 1)
    def _():
        landed(f_buf.at[pl.ds(0, 2 * lanes * depth)], f_send.at[0])
        landed(l_buf, l_send.at[0])

        @pl.when(crosses == 1)
        def _():
            landed(c_buf.at[0], c_send.at[1])
            landed(c_buf.at[pl.ds(0, 2)], c_send.at[2])

        @pl.when(crosses == 0)
        def _():
            landed(c_buf.at[0], c_send.at[2])

    for plane in range(line):
        @pl.when(z == plane)
        def _():
            if plane < line - 1:
                sent((plane + 1) * steps, send_z.at[0])
            if plane > 0:
                sent((line - plane) * steps, send_z.at[1])

    sent(line * last, send_y.at[0])
    landed(stats.at[pl.ds(0, n_ga - 1)], s_recv.at[0])
    everything = stats[0]
    for g in range(1, n_ga):
        everything = everything + stats[g]
    rms = jnp.sqrt(everything / (rows * n_ga) + 1e-06)
    rms_out[...] = rms
    scale = 1.0 / rms

    @pl.loop(0, 2)
    def _(t):
        part = pl.ds(pl.multiple_of(t * half, half), half)
        out[part, :] = (total[part, :] * scale).astype(jnp.bfloat16)

    landed(stats.at[pl.ds(0, n_ga - 1)], s_send.at[0])


def solution(mesh):
    n_ga, n_ba = mesh.shape["ga"], mesh.shape["ba"]
    line = 2 ** math.ceil(math.log2(n_ga) / 2)
    lanes = n_ga // line

    def edges(rows, width, depth, columns):
        dma = pltpu.SemaphoreType.DMA
        lent = columns // LENT // 128 * 128
        return functools.partial(edge_kernel, n_ga, n_ba, line, lent), [
            pltpu.VMEM((rows, columns), jnp.float32),
            pltpu.VMEM((n_ba, rows, width), jnp.bfloat16),
            pltpu.VMEM((n_ba - 1, rows, width), jnp.bfloat16),
            pltpu.VMEM((n_ga * depth, columns - lent), jnp.bfloat16),
            pltpu.VMEM((n_ga * depth, lent), jnp.bfloat16),
            pltpu.VMEM((rows, lent), jnp.float32),
            pltpu.VMEM((n_ga, 1, columns), jnp.float32),
            dma((line * PIECES,)),
            dma((2 * line,)),
            dma((line,)),
            dma((2,)),
            dma((2,)),
            dma((4,)),
            dma((2,)),
            dma((n_ba,)),
            dma((2,)),
            dma((3 * GIVEN,)),
            dma((3,)),
            dma((1,)),
            dma((1,)),
            dma((1,)),
            dma((1,)),
            dma((3,)),
        ], 59 * 2**20

    def plain(rows, width, depth, columns):
        dma = pltpu.SemaphoreType.DMA
        return functools.partial(kernel, n_ga, n_ba, line), [
            pltpu.VMEM((n_ba, rows, width), jnp.bfloat16),
            pltpu.VMEM((n_ga * depth, columns), jnp.bfloat16),
            pltpu.VMEM((n_ga, 1, columns), jnp.float32),
            dma((n_ga * CHUNKS,)),
            dma((2, line)),
            dma((2, n_ga)),
            dma((lanes - 1, line)),
            dma((n_ba,)),
            dma((n_ba // 2 - 1,)),
            dma((n_ba,)),
            dma((n_ga,)),
            dma((n_ga,)),
            dma((2,)),
        ], 48 * 2**20

    def body(coef, rot):
        rows, width = coef.shape
        depth, columns = rot.shape
        lends = (line, lanes, n_ba) == (4, 2, 4)
        run, scratch, limit = (edges if lends else plain)(rows, width, depth, columns)
        rotated, rms = pl.pallas_call(
            run,
            out_shape=(pltpu.VMEM((rows, columns), jnp.bfloat16 if lends else jnp.float32),
                       pltpu.VMEM((1, columns), jnp.float32)),
            in_specs=[pl.BlockSpec(memory_space=pltpu.HBM)] * 2,
            out_specs=(pl.BlockSpec(memory_space=pltpu.VMEM),) * 2,
            scratch_shapes=scratch,
            compiler_params=pltpu.CompilerParams(
                collective_id=0, has_side_effects=True, vmem_limit_bytes=limit),
        )(*(pltpu.with_memory_space_constraint(x, pltpu.HBM) for x in (coef, rot)))
        if not lends:
            rotated = (rotated * (1.0 / rms)).astype(jnp.bfloat16)
        return rotated, rms.reshape(columns)

    return jax.shard_map(body, mesh=mesh, in_specs=(P("ga", "ba"), P("ga", "ba")),
                         out_specs=(P("ga", "ba"), P("ba")), check_vma=False)
```

```python
import functools
import math

import jax
import jax.numpy as jnp
from jax import lax
from jax.experimental import pallas as pl
from jax.experimental.pallas import tpu as pltpu
from jax.sharding import PartitionSpec as P

MESH = pl.DeviceIdType.MESH
CHUNKS = 6
CROSS = 1
LENT = 6
MORE = 12


def kernel(n_ga, n_ba, line, coef, rot, total, rms_out, a_buf, b_buf, stats,
           recv, send_z, send_zb, send_y, a_recv, a_send_x, a_send_p, s_recv, s_send, own):
    lanes = n_ga // line
    depth = rot.shape[0]
    rows, width = coef.shape
    piece = depth // CHUNKS
    span = lanes * depth
    me, mb = lax.axis_index("ga"), lax.axis_index("ba")
    z, w = me // lanes, lax.rem(me, lanes)
    bx, bc = mb // 2, lax.rem(mb, 2)
    half = n_ba // 2

    def ga(i):
        return {"ga": i}

    def side(o):
        return lax.rem(w + o, lanes)

    def chunk(index):
        return b_buf.at[pl.ds(pl.multiple_of(index * piece, piece), piece)]

    partner = mb + 1 - 2 * bc
    far = [lax.rem(bx + o, half) * 2 + bc for o in range(1, half)]

    barrier = pltpu.get_barrier_semaphore()
    def greet(device):
        pl.semaphore_signal(barrier, inc=1, device_id=device, device_id_type=MESH)

    @pl.when(z > 0)
    def _():
        greet(ga(me - lanes))

    @pl.when(z < line - 1)
    def _():
        greet(ga(me + lanes))

    for o in range(1, lanes):
        greet(ga(z * lanes + side(o)))
    for target in [*far, partner]:
        greet({"ba": target})

    mine = [
        pltpu.make_async_copy(rot, b_buf.at[pl.ds(pl.multiple_of(me * depth, depth), depth)], own.at[0]),
        pltpu.make_async_copy(coef, a_buf.at[mb], own.at[1]),
    ]
    ends = (line - 1 - z) // (line - 1) + z // (line - 1)
    pl.semaphore_wait(barrier, 2 - ends + lanes - 1 + len(far) + 1)

    def remote(src, index, sem, target):
        return pltpu.make_async_remote_copy(
            src_ref=src, dst_ref=chunk(index), send_sem=sem, recv_sem=recv.at[index],
            device_id=ga(target), device_id_type=MESH)

    def arrived(index):
        pltpu.make_async_copy(chunk(index), chunk(index), recv.at[index]).wait()

    def along(k, src, index, sem):
        @pl.when(z < line - 1 if k == 0 else z > 0)
        def _():
            remote(src, index, sem, me + lanes if k == 0 else me - lanes).start()

    def across(src, index, from_z):
        for o in range(1, lanes):
            remote(src, index, send_y.at[o - 1, from_z], z * lanes + side(o)).start()

    def own_chunk(q):
        return rot.at[pl.ds(q * piece, piece)]

    last = CHUNKS - CROSS
    crossed = [(o, q) for q in range(last, CHUNKS) for o in range(1, lanes)]
    for q in range(last, CHUNKS):
        across(own_chunk(q), me * CHUNKS + q, z)
    for q in range(CHUNKS):
        for k in range(2):
            along(k, own_chunk(q), me * CHUNKS + q, send_z.at[k, z])
        if q < last:
            across(own_chunk(q), me * CHUNKS + q, z)

    def a_copy(src, index, sem, target):
        return pltpu.make_async_remote_copy(
            src_ref=src, dst_ref=a_buf.at[index], send_sem=sem, recv_sem=a_recv.at[index],
            device_id={"ba": target}, device_id_type=MESH)

    for o, target in enumerate(far):
        a_copy(coef, mb, a_send_x.at[o], target).start()
    a_copy(coef, mb, a_send_p.at[mb], partner).start()
    for copy in mine:
        copy.start()

    for o, q in crossed:
        index = (z * lanes + side(o)) * CHUNKS + q
        arrived(index)
        for k in range(2):
            along(k, chunk(index), index, send_zb.at[k, z * lanes + side(o)])

    tile = math.gcd(rows, 1280)

    def multiply(j, dist, part):
        from_z = z - dist + 2 * dist * j

        @pl.when((from_z >= 0) & (from_z < line) & ((dist > 0) | (j == 0)))
        def _():
            if part == "all":
                for o in range(1, lanes):
                    for q in range(last):
                        arrived((from_z * lanes + side(o)) * CHUNKS + q)
                panel(from_z * span, span, dist)
                return
            if part == "own":
                panel((from_z * lanes + w) * depth, depth, dist)
                return
            for o in range(1, lanes):
                block = from_z * lanes + side(o)
                for q in range(cut) if part == "cut" else range(cut, last):
                    arrived(block * CHUNKS + q)
                if part == "cut":
                    panel(block * depth, cut * piece, dist)
                else:
                    panel(block * depth + cut * piece, depth - cut * piece, dist)

    cut = max(q for q in range(last) if q * piece % 128 == 0) if depth % 128 == 0 else 0

    def panel(begin, size, dist):
        at, column = begin // width, pl.multiple_of(lax.rem(begin, width), 128)

        @pl.loop(0, rows // tile)
        def _(t):
            part = pl.ds(pl.multiple_of(t * tile, tile), tile)
            product = jnp.dot(
                a_buf[at, part, pl.ds(column, size)],
                b_buf[pl.ds(pl.multiple_of(begin, 128), size), :],
                preferred_element_type=jnp.float32)

            @pl.when(dist == 0)
            def _():
                total[part, :] = product

            @pl.when(dist > 0)
            def _():
                total[part, :] += product

    def at_distance(dist, part="all"):
        if cut == 0:
            if part in ("own", "cut"):
                return
            part = "all"
        lax.fori_loop(0, 2, lambda j, c: (multiply(j, dist, part), c)[1], 0)

    def relay(d, carry):
        for step, (o, q) in enumerate([(0, q) for q in range(CHUNKS)] + crossed):
            for k in range(2):
                from_z = z - d if k == 0 else z + d

                @pl.when((from_z >= 0) & (from_z < line))
                def _():
                    block = from_z * lanes + side(o)
                    index = block * CHUNKS + q
                    arrived(index)
                    along(k, chunk(index), index, send_zb.at[k, block] if o else send_z.at[k, from_z])
                    if q < last:
                        across(chunk(index), index, from_z)

            if step == CHUNKS // 3:
                @pl.when(d == 2)
                def _():
                    for source in far:
                        pltpu.make_async_copy(a_buf.at[source], a_buf.at[source], a_recv.at[source]).wait()
                        a_copy(a_buf.at[source], source, a_send_p.at[source], partner).start()

            if step == CHUNKS // 6:
                @pl.when(d == line - 1)
                def _():
                    at_distance(line - 3)

            for when, dist, part in ((CHUNKS // 2, line - 2, "own"), (CHUNKS - 2, line - 2, "cut"),
                                     (CHUNKS - 2, line - 2, "rest"), (CHUNKS - 1, line - 1, "own"),
                                     (CHUNKS - 1, line - 1, "cut")):
                if step == when:
                    @pl.when(d == line - 1)
                    def _():
                        at_distance(dist, part)

            if step == CHUNKS - 1:
                @pl.when(d == 2)
                def _():
                    for copy in mine:
                        copy.wait()
                    for x in range(half):
                        source = x * 2 + 1 - bc
                        pltpu.make_async_copy(a_buf.at[source], a_buf.at[source], a_recv.at[source]).wait()

                @pl.when((d >= 2) & (d < line - 1))
                def _():
                    at_distance(d - 2)
        return carry

    lax.fori_loop(1, line, relay, 0)
    at_distance(line - 1, "rest")

    def squares(t, c):
        v = total[pl.ds(pl.multiple_of(t * tile, tile), tile), :]
        return c + jnp.sum(v * v, axis=0, keepdims=True)

    stats[me] = lax.fori_loop(0, rows // tile, squares, jnp.zeros((1, total.shape[1]), jnp.float32))

    def share(o, target, slot):
        return pltpu.make_async_remote_copy(
            src_ref=stats.at[me], dst_ref=stats.at[me], send_sem=s_send.at[o], recv_sem=s_recv.at[slot],
            device_id=ga(target), device_id_type=MESH)

    for o in range(1, n_ga):
        share(o, lax.rem(me + o, n_ga), me).start()
    for o in range(1, n_ga):
        source = lax.rem(me + o, n_ga)
        pltpu.make_async_copy(stats.at[source], stats.at[source], s_recv.at[source]).wait()
    everything = stats[0]
    for g in range(1, n_ga):
        everything = everything + stats[g]
    rms = jnp.sqrt(everything / (rows * n_ga) + 1e-06)
    rms_out[...] = rms
    for o in range(1, n_ga):
        share(o, lax.rem(me + o, n_ga), me).wait_send()
    for o, target in enumerate(far):
        a_copy(coef, mb, a_send_x.at[o], target).wait_send()
    for x in range(half):
        a_copy(coef, x * 2 + bc, a_send_p.at[x * 2 + bc], partner).wait_send()

    def sent(count, sem):
        view = b_buf.at[pl.ds(0, count * piece)]
        pltpu.make_async_copy(view, view, sem).wait()

    for from_z in range(line):
        for k in range(2):
            @pl.when((z >= from_z) & (z < line - 1) if k == 0 else (z <= from_z) & (z > 0))
            def _():
                sent(CHUNKS, send_z.at[k, from_z])
                for o in range(1, lanes):
                    sent(CROSS, send_zb.at[k, from_z * lanes + side(o)])
        for o in range(1, lanes):
            @pl.when(z == from_z)
            def _():
                sent(CHUNKS, send_y.at[o - 1, from_z])

            @pl.when(z != from_z)
            def _():
                sent(last, send_y.at[o - 1, from_z])


PIECES = 12
GIVEN = 20


def edge_kernel(n_ga, n_ba, line, widths, coef, rot, out, rms_out, total, a_buf, c_buf, b_buf, f_buf, g_buf, l_buf, m_buf, stats,
                recv, recv_y, recv_x, send_z, send_y, f_recv, f_send, a_recv, a_send,
                c_recv, c_send, l_recv, l_send, s_recv, s_send, own):
    lanes = n_ga // line
    depth = rot.shape[0]
    rows, width = coef.shape
    lent = sum(widths)
    kept = rot.shape[1] - lent
    groups = ((f_buf, l_buf, 0, widths[0]), (g_buf, m_buf, widths[0], widths[1]))
    piece = depth // PIECES
    given = rows // GIVEN
    last = PIECES - 1
    half = rows // 2
    me, mb = lax.axis_index("ga"), lax.axis_index("ba")
    z, w = me // lanes, lax.rem(me, lanes)
    v = 1 - w
    bx, bc = mb // 2, lax.rem(mb, 2)
    partner = mb + 1 - 2 * bc
    far = (1 - bx) * 2 + bc
    beyond = (1 - bx) * 2 + 1 - bc
    inside = lax.rem((z + 1) // 2, 2)
    upper = z // (line // 2)
    mate = z + 1 - 2 * lax.rem(z, 2)
    toward = z + 1 - 2 * upper
    skip = upper * (line - 1)
    sx, sc = skip // 2, lax.rem(skip, 2)
    crosses = bc + sc - 2 * bc * sc
    late = (1 - crosses) * (1 - bx - sx + 2 * bx * sx)
    entry = mb + late * (far - mb)

    def ga(i):
        return {"ga": i}

    def ba(i):
        return {"ba": i}

    def remote(src, dst, send, arrive, target):
        return pltpu.make_async_remote_copy(
            src_ref=src, dst_ref=dst, send_sem=send, recv_sem=arrive, device_id=target, device_id_type=MESH)

    def landed(ref, sem):
        pltpu.make_async_copy(ref, ref, sem).wait()

    barrier = pltpu.get_barrier_semaphore()
    def greet(device):
        pl.semaphore_signal(barrier, inc=1, device_id=device, device_id_type=MESH)

    @pl.when(z > 0)
    def _():
        greet(ga(me - lanes))

    @pl.when(z < line - 1)
    def _():
        greet(ga(me + lanes))

    greet(ga(z * lanes + v))
    greet(ba(far))
    greet(ba(partner))

    mine = [
        pltpu.make_async_copy(
            rot.at[:, pl.ds(lent, kept)], b_buf.at[pl.ds(pl.multiple_of(me * depth, depth), depth)], own.at[0]),
        pltpu.make_async_copy(coef, a_buf.at[mb], own.at[1]),
    ] + [
        pltpu.make_async_copy(
            rot.at[:, pl.ds(begin, size)], held.at[pl.ds(pl.multiple_of(me * depth, depth), depth)], own.at[2 + g])
        for g, (held, _, begin, size) in enumerate(groups)
    ]
    ends = (line - 1 - z) // (line - 1) + z // (line - 1)
    pl.semaphore_wait(barrier, 2 - ends + 3)

    def chunk(index):
        return b_buf.at[pl.ds(pl.multiple_of(index * piece, piece), piece)]

    cut = last * piece // 256 * 256
    early = cut // piece

    def along(k, src, index, arrive):
        @pl.when(z < line - 1 if k == 0 else z > 0)
        def _():
            remote(src, chunk(index), send_z.at[k], arrive, ga(me + lanes if k == 0 else me - lanes)).start()

    def across(src, from_z, q):
        index = (from_z * lanes + w) * PIECES + q
        slot = from_z * 2 + q // early
        remote(src, chunk(index), send_y.at[0], recv_y.at[slot], ga(z * lanes + v)).start()

    def crossed_over(block, part):
        def wait(begin, end):
            view = b_buf.at[pl.ds(pl.multiple_of(block * depth + begin * piece, piece), (end - begin) * piece)]
            landed(view, recv_y.at[block // lanes * 2 + part])

        if part == 0:
            wait(0, early)
            return
        gap = (z - block // lanes) * (z - block // lanes)

        @pl.when(gap < 2)
        def _():
            wait(early, last)

        @pl.when(gap >= 2)
        def _():
            wait(early, PIECES)

    def own_chunk(q):
        return rot.at[pl.ds(q * piece, piece), pl.ds(lent, kept)]

    def f_block(g, block):
        return groups[g][0].at[pl.ds(pl.multiple_of(block * depth, depth), depth)]

    def f_arrived(g, block, slot):
        landed(f_block(g, block), f_recv.at[4 * g + slot])

    def f_along(g, src, block, slot):
        arrive = f_recv.at[4 * g + slot + inside * (3 - slot)]
        remote(src, f_block(g, block), f_send.at[g], arrive, ga(toward * lanes + w)).start()

    def f_pass(g, block, slot, later):
        f_arrived(g, block, slot)
        f_along(g, f_block(g, block), block, later)

    f_own = [rot.at[:, pl.ds(begin, size)] for _, _, begin, size in groups]
    f_over = [
        remote(f_own[g], f_block(g, me), f_send.at[2 + g], f_recv.at[4 * g], ga(z * lanes + v)) for g in range(2)]
    f_over[0].start()
    over = remote(own_chunk(last), chunk(me * PIECES + last), send_y.at[1], recv_x.at[z], ga(z * lanes + v))
    over.start()
    f_over[1].start()
    f_along(0, f_own[0], me, 1)
    for q in range(PIECES):
        for k in range(2):
            along(k, own_chunk(q), me * PIECES + q, recv.at[z * PIECES + q])
        if q < last:
            across(own_chunk(q), z, q)

    def a_copy(src, index, sem, target):
        return remote(src, a_buf.at[index], sem, a_recv.at[index], ba(target))

    a_copy(coef, mb, a_send.at[0], far).start()
    a_copy(coef, mb, a_send.at[1], partner).start()
    for copy in mine:
        copy.start()

    total[...] = jnp.zeros_like(total)
    side = z * lanes + v
    f_pass(0, side, 0, 2)
    landed(chunk(side * PIECES + last), recv_x.at[z])
    for k in range(2):
        along(k, chunk(side * PIECES + last), side * PIECES + last, recv_x.at[z])

    def strip(r):
        return pl.ds(pl.multiple_of(r * given, given), given)

    def c_at(block, r):
        return c_buf.at[block - 1 + upper, strip(r)]

    def c_copy(src, block, r, kind, sem, target):
        return remote(src, c_at(block, r), c_send.at[sem], c_recv.at[kind * GIVEN + r], target)

    def lend(source):
        @pl.loop(0, GIVEN)
        def _(r):
            c_copy(source.at[strip(r)], entry, r, 0, 0, ga(mate * lanes + w)).start()

    def second():
        f_along(1, f_own[1], me, 1)
        f_pass(1, side, 0, 2)

    @pl.when(inside == 0)
    def _():
        second()

    @pl.when((inside == 0) & (late == 0))
    def _():
        lend(coef)

    @pl.when(inside == 1)
    def _():
        f_pass(0, mate * lanes + w, 1, 3)

    def pass_entry(r):
        landed(c_at(entry, r), c_recv.at[r])

        @pl.when(crosses == 1)
        def _():
            c_copy(c_at(entry, r), entry, r, 1, 1, ba(far)).start()

        c_copy(c_at(entry, r), entry, r, 2, 2, ba(partner)).start()

    def pass_far(r):
        @pl.when(crosses == 1)
        def _():
            landed(c_at(far, r), c_recv.at[GIVEN + r])
            c_copy(c_at(far, r), far, r, 2, 2, ba(partner)).start()

    def both(job, r):
        job(2 * r)
        job(2 * r + 1)

    def ready():
        for copy in mine:
            copy.wait()
        for source in (partner, beyond):
            landed(a_buf.at[source], a_recv.at[source])

    def order(i):
        j, lane = i // lanes, lax.rem(i, lanes)
        near = j + inside * (1 - j // 2) * (1 - 2 * lax.rem(j, 2))
        from_z = near + upper * (line - 1 - 2 * near)
        return from_z * lanes + w + lane * (1 - 2 * w), lane

    def panel(begin, size):
        at, column = begin // width, pl.multiple_of(lax.rem(begin, width), 128)

        @pl.loop(0, 2)
        def _(t):
            part = pl.ds(pl.multiple_of(t * half, half), half)
            total[part, pl.ds(lent, kept)] += jnp.dot(
                a_buf[at, part, pl.ds(column, size)],
                b_buf[pl.ds(pl.multiple_of(begin, 128), size), :],
                preferred_element_type=jnp.float32)

    def whole(i):
        block, lane = order(i)

        @pl.when(lane == 1)
        def _():
            crossed_over(block, 0)
            crossed_over(block, 1)

        panel(block * depth, depth)

    steps = PIECES + 1

    @pl.loop(0, (line - 1) * steps)
    def _(t):
        d, step = 1 + t // steps, lax.rem(t, steps)
        crossed = step // PIECES
        q = step - crossed

        @pl.when((inside == 1) & (d == 1) & (step == PIECES))
        def _():
            f_pass(0, mate * lanes + v, 2, 3)

        @pl.when((inside == 1) & (d == 2) & (step == 0))
        def _():
            second()
            f_pass(1, mate * lanes + w, 1, 3)
            f_pass(1, mate * lanes + v, 2, 3)

        for k in range(2):
            from_z = z - d if k == 0 else z + d

            @pl.when((from_z >= 0) & (from_z < line))
            def _():
                @pl.when(crossed == 0)
                def _():
                    index = (from_z * lanes + w) * PIECES + q
                    sem = recv.at[from_z * PIECES + q]
                    landed(chunk(index), sem)
                    along(k, chunk(index), index, sem)

                    @pl.when((q < last) | (d > 1))
                    def _():
                        across(chunk(index), from_z, q)

                @pl.when((crossed == 1) & (d == 1))
                def _():
                    landed(chunk((from_z * lanes + v) * PIECES + last), recv_x.at[from_z])

        @pl.when((d == 2) & (step == inside * 4 + (1 - inside) * PIECES))
        def _():
            landed(a_buf.at[far], a_recv.at[far])
            a_copy(a_buf.at[far], far, a_send.at[1], partner).start()

            @pl.when((inside == 0) & (late == 1))
            def _():
                lend(a_buf.at[far])

        @pl.when((inside == 1) & (d == 2) & (step > 2) & (step < 10) & (lax.rem(step, 2) == 1))
        def _():
            r = step // 2 - 1

            @pl.when(late == 0)
            def _():
                both(pass_entry, r)

            @pl.when(r >= 3)
            def _():
                both(pass_far, r - 3)

        turn = step - inside * 6 - (1 - inside) * 2

        @pl.when((d == 3 - inside) & (turn >= 0) & (turn < 6) & (lax.rem(turn + 8, 2) == 0))
        def _():
            n = turn // 2

            @pl.when(n == 0)
            def _():
                ready()

            whole(n)

    def lent_product(source, part, held, begin, count):
        product = jnp.dot(
            source[0, part, :], held[pl.ds(begin, width), :], preferred_element_type=jnp.float32)
        for s in range(1, count):
            product += jnp.dot(
                source[s, part, :], held[pl.ds(begin + s * width, width), :], preferred_element_type=jnp.float32)
        return product

    def answer(g, r, count=2):
        held, back, _, _ = groups[g]
        part = pl.ds(pl.multiple_of(r * count * given, given), count * given)
        back[part, :] = lent_product(
            c_buf, part, held, pl.multiple_of((1 - upper) * width, width), n_ba - 1)
        remote(back.at[part], back.at[part], l_send.at[g], l_recv.at[g], ga(mate * lanes + w)).start()

    def joined(r):
        both(joined_half, r)

    def joined_half(r):
        @pl.when(crosses == 1)
        def _():
            landed(c_at((1 - sx) * 2 + sc, r), c_recv.at[2 * GIVEN + r])

        @pl.when(crosses == 0)
        def _():
            landed(c_buf.at[pl.ds(0, 2), strip(r)], c_recv.at[2 * GIVEN + r])

    def serve(at, prompt=(), slow=(), distant=()):
        for condition, jobs, job in ((late == 0, prompt, pass_entry), (late == 1, slow, pass_entry), (True, distant, pass_far)):
            for when, which in jobs:
                @pl.when((at == when) & condition)
                def _():
                    both(job, which)

    def all_here(g):
        landed(groups[g][0].at[pl.ds(0, 2 * lanes * depth)], f_recv.at[4 * g + 3])

    def own_lent(g):
        held, _, begin, size = groups[g]

        def compute(t):
            part = pl.ds(pl.multiple_of(t * half, half), half)
            total[part, pl.ds(begin, size)] = lent_product(a_buf, part, held, 0, n_ba)
        return compute

    @pl.loop(0, 4)
    def _(j):
        @pl.when((inside == 1) & (j == 1))
        def _():
            serve(j, prompt=((1, 4),), distant=((1, 1), (1, 2)))

        @pl.when((inside == 1) & (j == 2))
        def _():
            all_here(0)

            @pl.loop(0, 4)
            def _(r):
                serve(r, slow=((0, 0), (1, 1), (2, 2), (3, 3)), distant=((0, 3), (1, 4)))
                joined(r)
                answer(0, r)

            serve(j, prompt=((2, 5),))
            pl.loop(0, 2)(own_lent(0))

        @pl.when((inside == 1) & (j >= 2))
        def _():
            serve(j, prompt=((2, 6), (3, 7)), slow=((2, 4), (3, 5)), distant=((2, 5), (3, 6)))
            joined(j + 2)
            answer(0, j + 2)

            @pl.when(j == 2)
            def _():
                all_here(1)

            @pl.loop(4 * j - 8, 2 * j)
            def _(r):
                answer(1, r)

            @pl.when(j == 3)
            def _():
                serve(j, slow=((3, 6),))
                joined(6)
                answer(0, 6)
                answer(1, 6)
                pl.loop(0, 2)(own_lent(1))
                serve(j, prompt=((3, 8),), slow=((3, 7),), distant=((3, 7),))

        whole(4 + 2 * j - j // 2 * 5)

    @pl.when(inside == 0)
    def _():
        for held, _, begin, size in groups:
            @pl.loop(0, 2)
            def _(t):
                part = pl.ds(pl.multiple_of(t * half, half), half)
                total[part, pl.ds(begin, size)] = jnp.dot(
                    a_buf[skip, part, :], held[pl.ds(pl.multiple_of(skip * width, width), width), :],
                    preferred_element_type=jnp.float32)

    @pl.when(inside == 1)
    def _():
        @pl.loop(7, 9)
        def _(r):
            serve(r, slow=((7, 8),))

            @pl.when(r == 8)
            def _():
                pass_entry(18)

            serve(r, distant=((8, 8),))
            joined(r)
            answer(0, r)
            answer(1, r)

        pass_entry(19)

        @pl.loop(18, 20)
        def _(r):
            pass_far(r)
            joined_half(r)
            answer(0, r, 1)
            answer(1, r, 1)

    final, _ = order(7)
    crossed_over(final, 0)
    panel(final * depth, cut)

    @pl.when(inside == 0)
    def _():
        for g, (_, back, begin, size) in enumerate(groups):
            landed(back, l_recv.at[g])
            total[:, pl.ds(begin, size)] += back[...]

    lent_part = total[:, pl.ds(0, lent)]
    stats[me, :, pl.ds(0, lent)] = jnp.sum(lent_part * lent_part, axis=0, keepdims=True)
    crossed_over(final, 1)
    begin = final * depth + cut
    at, column = begin // width, pl.multiple_of(lax.rem(begin, width), 128)

    def finish(t, squares):
        part = pl.ds(pl.multiple_of(t * half, half), half)
        done = total[part, pl.ds(lent, kept)] + jnp.dot(
            a_buf[at, part, pl.ds(column, depth - cut)],
            b_buf[pl.ds(pl.multiple_of(begin, 128), depth - cut), :],
            preferred_element_type=jnp.float32)
        total[part, pl.ds(lent, kept)] = done
        return squares + jnp.sum(done * done, axis=0, keepdims=True)

    stats[me, :, pl.ds(lent, kept)] = lax.fori_loop(0, 2, finish, jnp.zeros((1, kept), jnp.float32))

    def share(target):
        return remote(stats.at[me], stats.at[me], s_send.at[0], s_recv.at[0], ga(target))

    planes = (line - 1 - z, lax.rem(z + line // 2, line), mate)
    others = [plane * lanes + lane for plane in planes for lane in (v, w)] + [z * lanes + v]
    for target in others:
        share(target).start()

    def sent(count, sem):
        landed(b_buf.at[pl.ds(0, count * piece)], sem)

    landed(a_buf.at[0], a_send.at[0])
    landed(a_buf.at[pl.ds(0, 2)], a_send.at[1])
    for g in range(2):
        f_over[g].wait_send()
    over.wait_send()

    @pl.when(inside == 0)
    def _():
        for g in range(2):
            landed(groups[g][0].at[pl.ds(0, lanes * depth)], f_send.at[g])
        landed(c_buf.at[0], c_send.at[0])

    @pl.when(inside == 1)
    def _():
        for g in range(2):
            landed(groups[g][0].at[pl.ds(0, 2 * lanes * depth)], f_send.at[g])
            landed(groups[g][1], l_send.at[g])

        @pl.when(crosses == 1)
        def _():
            landed(c_buf.at[0], c_send.at[1])
            landed(c_buf.at[pl.ds(0, 2)], c_send.at[2])

        @pl.when(crosses == 0)
        def _():
            landed(c_buf.at[0], c_send.at[2])

    for plane in range(line):
        @pl.when(z == plane)
        def _():
            if plane < line - 1:
                sent((plane + 1) * PIECES + 1, send_z.at[0])
            if plane > 0:
                sent((line - plane) * PIECES + 1, send_z.at[1])
            sent(line * last + sum(abs(plane - other) > 1 for other in range(line)), send_y.at[0])

    landed(stats.at[pl.ds(0, n_ga - 1)], s_recv.at[0])
    everything = stats[0]
    for g in range(1, n_ga):
        everything = everything + stats[g]
    rms = jnp.sqrt(everything / (rows * n_ga) + 1e-06)
    rms_out[...] = rms
    scale = 1.0 / rms

    @pl.loop(0, 2)
    def _(t):
        part = pl.ds(pl.multiple_of(t * half, half), half)
        out[part, :] = (total[part, :] * scale).astype(jnp.bfloat16)

    landed(stats.at[pl.ds(0, n_ga - 1)], s_send.at[0])


def solution(mesh):
    n_ga, n_ba = mesh.shape["ga"], mesh.shape["ba"]
    line = 2 ** math.ceil(math.log2(n_ga) / 2)
    lanes = n_ga // line

    def edges(rows, width, depth, columns):
        dma = pltpu.SemaphoreType.DMA
        widths = columns // LENT // 128 * 128, columns // MORE // 128 * 128
        return functools.partial(edge_kernel, n_ga, n_ba, line, widths), [
            pltpu.VMEM((rows, columns), jnp.float32),
            pltpu.VMEM((n_ba, rows, width), jnp.bfloat16),
            pltpu.VMEM((n_ba - 1, rows, width), jnp.bfloat16),
            pltpu.VMEM((n_ga * depth, columns - sum(widths)), jnp.bfloat16),
            *(pltpu.VMEM((n_ga * depth, size), jnp.bfloat16) for size in widths),
            *(pltpu.VMEM((rows, size), jnp.float32) for size in widths),
            pltpu.VMEM((n_ga, 1, columns), jnp.float32),
            dma((line * PIECES,)),
            dma((2 * line,)),
            dma((line,)),
            dma((2,)),
            dma((2,)),
            dma((8,)),
            dma((4,)),
            dma((n_ba,)),
            dma((2,)),
            dma((3 * GIVEN,)),
            dma((3,)),
            dma((2,)),
            dma((2,)),
            dma((1,)),
            dma((1,)),
            dma((4,)),
        ], 59 * 2**20

    def plain(rows, width, depth, columns):
        dma = pltpu.SemaphoreType.DMA
        return functools.partial(kernel, n_ga, n_ba, line), [
            pltpu.VMEM((n_ba, rows, width), jnp.bfloat16),
            pltpu.VMEM((n_ga * depth, columns), jnp.bfloat16),
            pltpu.VMEM((n_ga, 1, columns), jnp.float32),
            dma((n_ga * CHUNKS,)),
            dma((2, line)),
            dma((2, n_ga)),
            dma((lanes - 1, line)),
            dma((n_ba,)),
            dma((n_ba // 2 - 1,)),
            dma((n_ba,)),
            dma((n_ga,)),
            dma((n_ga,)),
            dma((2,)),
        ], 48 * 2**20

    def body(coef, rot):
        rows, width = coef.shape
        depth, columns = rot.shape
        lends = (line, lanes, n_ba) == (4, 2, 4)
        run, scratch, limit = (edges if lends else plain)(rows, width, depth, columns)
        rotated, rms = pl.pallas_call(
            run,
            out_shape=(pltpu.VMEM((rows, columns), jnp.bfloat16 if lends else jnp.float32),
                       pltpu.VMEM((1, columns), jnp.float32)),
            in_specs=[pl.BlockSpec(memory_space=pltpu.HBM)] * 2,
            out_specs=(pl.BlockSpec(memory_space=pltpu.VMEM),) * 2,
            scratch_shapes=scratch,
            compiler_params=pltpu.CompilerParams(
                collective_id=0, has_side_effects=True, vmem_limit_bytes=limit),
        )(*(pltpu.with_memory_space_constraint(x, pltpu.HBM) for x in (coef, rot)))
        if not lends:
            rotated = (rotated * (1.0 / rms)).astype(jnp.bfloat16)
        return rotated, rms.reshape(columns)

    return jax.shard_map(body, mesh=mesh, in_specs=(P("ga", "ba"), P("ga", "ba")),
                         out_specs=(P("ga", "ba"), P("ba")), check_vma=False)
```
